32 devices in a mesh: dp: 1 (over z), tp: 4 (over y), ep: 8 (over x, core).
Axes of the slice: x: 4, y: 4, z: 1, core: 2. Of those that a mesh axis runs over, the one named last changes fastest.
The devices are a block of a 4x4x8 slice.
Arguments:
- hidden: bfloat16 [16384, 2048], P(('dp', 'ep'))
- expert_ids: int32 [16384, 2], P(('dp', 'ep'))
- norm_w: bfloat16 [2048], replicated
- router_w: bfloat16 [2048, 8], replicated
- w_gate: bfloat16 [8, 2048, 5632], P('ep', None, 'tp')
- w_up: bfloat16 [8, 2048, 5632], P('ep', None, 'tp')
- w_down: bfloat16 [8, 5632, 2048], P('ep', 'tp')
Outputs:
- output: bfloat16 [16384, 2048], P(('dp', 'ep'))
All inputs are finite; a program needn't handle non-finite values.
Results may differ from the reference program's by a relative error of at most 0.0106688.
Values are sent between devices in bfloat16 or wider.
A program may use at most 768 MiB of HBM per device.

```python
import jax
import jax.numpy as jnp
from jax import lax

D = 2048
FF = 5632
EXPERTS = 8
TOP = 2
TOK_DEV = 2048
EP = 8
CAP = 1024
TOKENS = TOK_DEV * EP
NORM_EPS = 1e-6


def random_order(order_key, count):
    order_score = jax.random.randint(order_key, (count,), 0, count) * count + jnp.arange(count, dtype=jnp.int32)
    return jnp.argsort(order_score)


def draw_routes(route_key):
    pair_count = TOP * TOK_DEV
    weight_total = (EXPERTS - 1) * (5 * EXPERTS - 2) // 2
    bounds = [CAP + ((pair_count - CAP) * (4 * rank_step * (EXPERTS - 1) - 3 * rank_step * (rank_step - 1) // 2)) // weight_total for rank_step in range(EXPERTS - 1)]
    bound_arr = jnp.array(bounds, dtype=jnp.int32)
    positions = jnp.arange(TOK_DEV, dtype=jnp.int32)[:, None] + TOK_DEV * jnp.arange(TOP, dtype=jnp.int32)[None, :]
    rank_of = jnp.sum((positions[:, :, None] >= bound_arr).astype(jnp.int32), axis=-1)
    label_key, rows_key = jax.random.split(route_key)
    labels = random_order(label_key, EXPERTS).astype(jnp.int32)
    choices = labels[rank_of]
    row_keys = jax.random.split(rows_key, EP)
    orders = jax.vmap(lambda sub_key: random_order(sub_key, TOK_DEV))(row_keys)
    return choices[orders].reshape(TOKENS, TOP).astype(jnp.int32)


def setup_inputs(seed: int = 0, part: int = 0) -> dict:
    base_key = jax.random.key(seed)
    key_list = jax.random.split(base_key, 7)
    hidden = jax.random.normal(jax.random.fold_in(key_list[0], part), (TOKENS, D), jnp.float32)
    expert_ids = draw_routes(jax.random.fold_in(key_list[1], part))
    norm_w = 1.0 + 0.3 * jax.random.normal(key_list[2], (D,), jnp.float32)
    router_w = D ** -0.5 * jax.random.normal(key_list[3], (D, EXPERTS), jnp.float32)
    w_gate = D ** -0.5 * jax.random.normal(key_list[4], (EXPERTS, D, FF), jnp.float32)
    w_up = D ** -0.5 * jax.random.normal(key_list[5], (EXPERTS, D, FF), jnp.float32)
    down_scale = 2.0 * EXPERTS / (TOP * FF) ** 0.5
    w_down = down_scale * jax.random.normal(key_list[6], (EXPERTS, FF, D), jnp.float32)
    return {"hidden": hidden.astype(jnp.bfloat16), "expert_ids": expert_ids, "norm_w": norm_w.astype(jnp.bfloat16), "router_w": router_w.astype(jnp.bfloat16), "w_gate": w_gate.astype(jnp.bfloat16), "w_up": w_up.astype(jnp.bfloat16), "w_down": w_down.astype(jnp.bfloat16)}


def rms_norm(hidden, norm_w):
    wide_h = hidden.astype(jnp.float32)
    mean_sq = jnp.mean(wide_h * wide_h, axis=-1, keepdims=True)
    return (wide_h * lax.rsqrt(mean_sq + NORM_EPS) * norm_w.astype(jnp.float32)).astype(jnp.bfloat16)


def reference(hidden, expert_ids, norm_w, router_w, w_gate, w_up, w_down):
    normed = rms_norm(hidden, norm_w)
    logits = jnp.dot(normed, router_w, preferred_element_type=jnp.float32)
    router_prob = jax.nn.softmax(logits, axis=-1)
    gate_prob = jnp.take_along_axis(router_prob, expert_ids, axis=-1).reshape(-1)
    flat_ids = expert_ids.reshape(-1)
    pair_tok = jnp.arange(TOKENS * TOP, dtype=jnp.int32) // TOP
    row_limit = EP * CAP

    def one_expert(accum, per_expert):
        expert, gate_e, up_e, down_e = per_expert
        chosen = flat_ids == expert
        (picked,) = jnp.nonzero(chosen, size=row_limit, fill_value=0)
        row_valid = jnp.arange(row_limit) < jnp.sum(chosen.astype(jnp.int32))
        tok_rows = pair_tok[picked]
        x_rows = normed[tok_rows]
        gate_pre = jnp.dot(x_rows, gate_e, preferred_element_type=jnp.float32)
        up_pre = jnp.dot(x_rows, up_e, preferred_element_type=jnp.float32)
        act_rows = (jax.nn.silu(gate_pre) * up_pre).astype(jnp.bfloat16)
        expert_out = jnp.dot(act_rows, down_e, preferred_element_type=jnp.float32).astype(jnp.bfloat16)
        weight = jnp.where(row_valid, gate_prob[picked], 0.0)
        return accum.at[tok_rows].add(weight[:, None] * expert_out.astype(jnp.float32)), None

    moe_sum, _ = lax.scan(one_expert, jnp.zeros((TOKENS, D), jnp.float32), (jnp.arange(EXPERTS, dtype=jnp.int32), w_gate, w_up, w_down))
    return (hidden.astype(jnp.float32) + moe_sum).astype(jnp.bfloat16)
```

```python
import functools

import jax
import jax.numpy as jnp
from jax import lax
from jax.experimental import pallas as pl
from jax.experimental.pallas import tpu as pltpu
from jax.sharding import PartitionSpec as P

NORM_EPS = 1e-6
VMEM_LIMIT = 60 * 1024 * 1024
SLOT_TILE = 256
TOK_TILE = 512
RING = 4
MESH = pl.DeviceIdType.MESH
BLOCKS = ((0, 0), (0, 1), (-1, 0), (1, 0), (-1, 1), (1, 1), (2, 0), (2, 1))


def rms_norm(hidden, norm_w):
    wide_h = hidden.astype(jnp.float32)
    mean_sq = jnp.mean(wide_h * wide_h, axis=-1, keepdims=True)
    return (wide_h * lax.rsqrt(mean_sq + NORM_EPS) * norm_w.astype(jnp.float32)).astype(jnp.bfloat16)


def row_cap(tok_dev, top_k, n_experts):
    return 8 * ((2 * top_k * tok_dev + 8 * n_experts - 1) // (8 * n_experts))


def expert_kernel(chips, tp_size, v_ref, pos_ref, gate_hbm, up_hbm, down_hbm, vbuf, home,
                  gate_ref, up_ref, down_ref, v_now, pos_now, stage, recv_f, recv_c, recv_d, fin,
                  w_sem, v_sem, part_sem, hop_send, hop_recv, pair_send, pair_recv, fwd_send, fwd_recv,
                  f_send, f_recv, c_send, c_recv, d_send, d_recv, home_send, home_recv, own_sem):
    y = lax.axis_index("tp")
    me = lax.axis_index("ep")
    chip, core = me // 2, me % 2
    tok_dev = v_ref.shape[0]
    half, quarter = tok_dev // 2, tok_dev // 4
    n_tiles = home.shape[1] // SLOT_TILE
    steps = len(BLOCKS) * n_tiles
    wide = v_now.shape[1] // tp_size
    side = wide // 2
    to_ep = lambda dx, c: {"ep": 2 * lax.rem(chip + dx + chips, chips) + c}
    to_tp = lambda dy: {"tp": lax.rem(y + dy + tp_size, tp_size)}
    partner = to_ep(0, 1 - core)

    weights = [pltpu.make_async_copy(a, b, w_sem.at[j]) for j, (a, b) in enumerate(((gate_hbm, gate_ref), (up_hbm, up_ref), (down_hbm, down_ref)))]
    for w in weights:
        w.start()

    barrier = pltpu.get_barrier_semaphore()
    peers = [to_tp(1), to_tp(-1), partner] + [to_ep(dx, c) for dx in (-1, 1, 2) for c in (0, 1)]
    for peer in peers:
        pl.semaphore_signal(barrier, inc=1, device_id=peer, device_id_type=MESH)
    pl.semaphore_wait(barrier, len(peers))

    def remote(src, dst, send, recv, device):
        return pltpu.make_async_remote_copy(src_ref=src, dst_ref=dst, send_sem=send, recv_sem=recv, device_id=device, device_id_type=MESH)

    mine = pl.ds(pl.multiple_of(core * half, half), half)
    others = pl.ds(pl.multiple_of((1 - core) * half, half), half)

    def swap(j):
        rows = others if j == 0 else mine
        return remote(v_ref.at[rows], vbuf.at[0, rows], part_sem.at[0, j], part_sem.at[1, j], partner)

    def hop(sc, sign, own):
        src = v_ref.at[mine] if own else vbuf.at[0, mine]
        k = BLOCKS.index((-sign, sc)) - 1
        return remote(src, vbuf.at[k, mine], hop_send.at[sc, (sign + 1) // 2], hop_recv.at[sc, (sign + 1) // 2], to_ep(sign, core))

    def forward(sc, sign):
        rows = pl.ds(pl.multiple_of(core * half + (quarter if sign < 0 else 0), quarter), quarter)
        return remote(vbuf.at[BLOCKS.index((-sign, sc)) - 1, rows], vbuf.at[BLOCKS.index((2, sc)) - 1, rows], fwd_send.at[sc, (sign + 1) // 2], fwd_recv.at[sc, (sign + 1) // 2], to_ep(sign, core))

    def pair(k):
        return remote(vbuf.at[k - 1, mine], vbuf.at[k - 1, mine], pair_send.at[k], pair_recv.at[k], partner)

    def pair_arrival(k):
        return remote(vbuf.at[k - 1, others], vbuf.at[k - 1, others], pair_send.at[k], pair_recv.at[k], partner)

    swap(0).start()
    swap(1).start()

    @pl.when(core == 0)
    def _():
        hop(0, 1, True).start()
        hop(0, -1, True).start()

    @pl.when(core == 1)
    def _():
        remote(v_ref.at[mine], vbuf.at[0, mine], part_sem.at[0, 0], part_sem.at[1, 0], partner).wait_recv()
        hop(0, 1, False).start()
        hop(0, -1, False).start()
        hop(1, 1, True).start()
        hop(1, -1, True).start()

    @pl.when(core == 0)
    def _():
        remote(v_ref.at[mine], vbuf.at[0, mine], part_sem.at[0, 0], part_sem.at[1, 0], partner).wait_recv()
        hop(1, 1, False).start()
        hop(1, -1, False).start()

    def load(src, row):
        copy = pltpu.make_async_copy(src, v_now, v_sem)
        copy.start()
        pos_now[...] = pos_ref[pl.ds(row, 1), :]
        copy.wait()

    def block_start(k):
        dx, sc = BLOCKS[k]
        if k == 0:
            for w in weights:
                w.wait()
            load(v_ref, me)
            return
        if k == 1:
            remote(v_ref.at[others], vbuf.at[0, others], part_sem.at[0, 1], part_sem.at[1, 1], partner).wait_recv()
            load(vbuf.at[0], 2 * chip + 1 - core)
            return
        if k in (2, 4):
            for sign in (1, -1):
                hop(sc, sign, True).wait_recv()
                forward(sc, sign).start()
                pair(BLOCKS.index((-sign, sc))).start()
        if dx == 2:
            for sign in (1, -1):
                forward(sc, sign).wait_recv()
            pair(k).start()
        pair_arrival(k).wait_recv()
        load(vbuf.at[k - 1], 2 * lax.rem(chip + dx + chips, chips) + sc)

    def f_copy(s, d):
        return remote(stage.at[s, 3, d], recv_f.at[d, s], f_send.at[d, s], f_recv.at[d, s], to_tp(1 - 2 * d))

    def c_copy(s, d):
        return remote(stage.at[s, 1 + d, d], recv_c.at[d, s], c_send.at[d, s], c_recv.at[d, s], to_tp(1 - 2 * d))

    def d_copy(s, d):
        return remote(stage.at[s, 1 + d, 1 - d], recv_d.at[d, s], d_send.at[d, s], d_recv.at[d, s], to_tp(1 - 2 * d))

    def rows_of(tile):
        return pl.ds(pl.multiple_of(tile * SLOT_TILE, SLOT_TILE), SLOT_TILE)

    def home_copy(k, s, tile):
        dx, sc = BLOCKS[k]
        device = partner if k == 1 else to_ep(dx, sc)
        return remote(fin.at[s], home.at[me, rows_of(tile)], home_send.at[s], home_recv, device)

    def own_copy(s, tile):
        return pltpu.make_async_copy(fin.at[s], home.at[me, rows_of(tile)], own_sem.at[s])

    def step(i, carry):
        for k in range(len(BLOCKS)):
            @pl.when(i == k * n_tiles)
            def _(k=k):
                block_start(k)

        @pl.when(i < steps)
        def _():
            s = lax.rem(i, RING)

            @pl.when(i >= RING)
            def _():
                for d in (0, 1):
                    f_copy(s, d).wait_send()
                    c_copy(s, d).wait_send()
                    d_copy(s, d).wait_send()

            slots = lax.rem(i, n_tiles) * SLOT_TILE + lax.broadcasted_iota(jnp.int32, (SLOT_TILE, tok_dev), 0)
            pick = jnp.where(pos_now[...] == slots, 1.0, 0.0).astype(jnp.bfloat16)
            rows = jnp.dot(pick, v_now[...], preferred_element_type=jnp.float32).astype(jnp.bfloat16)
            gate_pre = jnp.dot(rows, gate_ref[...], preferred_element_type=jnp.float32)
            up_pre = jnp.dot(rows, up_ref[...], preferred_element_type=jnp.float32)
            act = (jax.nn.silu(gate_pre) * up_pre).astype(jnp.bfloat16)
            for part, dy in ((3, 2), (1, 1), (2, -1), (0, 0)):
                q = lax.rem(y + dy + tp_size, tp_size)
                for d in (0, 1):
                    cols = pl.ds(pl.multiple_of(q * wide + d * side, side), side)
                    stage[s, part, d] = jnp.dot(act, down_ref[:, cols], preferred_element_type=jnp.float32).astype(jnp.bfloat16)
            for d in (0, 1):
                f_copy(s, d).start()
            for d in (0, 1):
                d_copy(s, d).start()

        @pl.when(i >= 2)
        def _():
            j = i - 2
            s = lax.rem(j, RING)
            tile = lax.rem(j, n_tiles)
            for d in (0, 1):
                c_copy(s, d).wait_recv()
                d_copy(s, d).wait_recv()

            @pl.when((j >= RING) & (j < RING + n_tiles))
            def _():
                own_copy(s, tile).wait()

            @pl.when(j >= RING + n_tiles)
            def _():
                home_copy(2, s, tile).wait_send()

            f32 = lambda a: a.astype(jnp.float32)
            for d in (0, 1):
                total = f32(stage[s, 0, d]) + f32(recv_c[d, s]) + f32(recv_d[1 - d, s])
                fin[s, :, d * side:(d + 1) * side] = total.astype(jnp.bfloat16)

            @pl.when(j < n_tiles)
            def _():
                own_copy(s, tile).start()

            for k in range(1, len(BLOCKS)):
                @pl.when(j // n_tiles == k)
                def _(k=k):
                    home_copy(k, s, tile).start()

        @pl.when((i >= 1) & (i <= steps))
        def _():
            s = lax.rem(i - 1, RING)
            for d in (0, 1):
                f_copy(s, d).wait_recv()
                stage[s, 1 + d, d] = (stage[s, 1 + d, d].astype(jnp.float32) + recv_f[d, s].astype(jnp.float32)).astype(jnp.bfloat16)
                c_copy(s, d).start()

        return carry

    assert n_tiles == RING
    lax.fori_loop(0, steps + 2, step, 0)

    for s in range(RING):
        for d in (0, 1):
            f_copy(s, d).wait_send()
            c_copy(s, d).wait_send()
            d_copy(s, d).wait_send()
        home_copy(2, s, s).wait_send()
    for j in (0, 1):
        swap(j).wait_send()
    for sc in (0, 1):
        for sign in (1, -1):
            hop(sc, sign, True).wait_send()
            forward(sc, sign).wait_send()
    for k in range(2, len(BLOCKS)):
        pair(k).wait_send()
    arrived = home.at[pl.ds(0, home.shape[0] - 1)]
    remote(arrived, arrived, home_send.at[0], home_recv, partner).wait_recv()


def experts_apply(chips, tp_size, row_limit, v, pos_rows, gate, up, down):
    tok_dev, dim = v.shape
    ff = gate.shape[1]
    width = dim // tp_size
    side = width // 2
    n = len(BLOCKS)
    bf16 = jnp.bfloat16
    anywhere = pl.BlockSpec(memory_space=pl.ANY)
    dma = pltpu.SemaphoreType.DMA
    ring = (2, RING, SLOT_TILE, side)
    return pl.pallas_call(
        functools.partial(expert_kernel, chips, tp_size),
        out_shape=(jax.ShapeDtypeStruct((n - 1, tok_dev, dim), bf16), jax.ShapeDtypeStruct((n, row_limit, width), bf16)),
        in_specs=[anywhere, pl.BlockSpec(memory_space=pltpu.VMEM), anywhere, anywhere, anywhere],
        out_specs=(anywhere, anywhere),
        scratch_shapes=[
            pltpu.VMEM((dim, ff), bf16), pltpu.VMEM((dim, ff), bf16), pltpu.VMEM((ff, dim), bf16),
            pltpu.VMEM((tok_dev, dim), bf16), pltpu.VMEM((1, tok_dev), jnp.int32),
            pltpu.VMEM((RING, 4, 2, SLOT_TILE, side), bf16), pltpu.VMEM(ring, bf16), pltpu.VMEM(ring, bf16), pltpu.VMEM(ring, bf16),
            pltpu.VMEM((RING, SLOT_TILE, width), bf16),
            dma((3,)), dma, dma((2, 2)), dma((2, 2)), dma((2, 2)), dma((n,)), dma((n,)), dma((2, 2)), dma((2, 2)),
            dma((2, RING)), dma((2, RING)), dma((2, RING)), dma((2, RING)), dma((2, RING)), dma((2, RING)),
            dma((RING,)), dma, dma((RING,)),
        ],
        cost_estimate=pl.CostEstimate(flops=2 * n * row_limit * dim * (tok_dev + 3 * ff), bytes_accessed=2 * (n * tok_dev * dim + 3 * dim * ff), transcendentals=n * row_limit * ff),
        compiler_params=pltpu.CompilerParams(collective_id=0, has_side_effects=True, vmem_limit_bytes=VMEM_LIMIT),
        name="experts",
    )(v, pos_rows, gate, up, down)[1]


def combine_kernel(hidden_ref, pos_ref, prob_ref, y_ref, out_ref):
    acc = hidden_ref[...].astype(jnp.float32)
    for e in range(y_ref.shape[0]):
        slots = lax.broadcasted_iota(jnp.int32, (acc.shape[0], y_ref.shape[1]), 1)
        pick = jnp.where(pos_ref[:, e:e + 1] == slots, 1.0, 0.0).astype(jnp.bfloat16)
        acc += prob_ref[:, e:e + 1] * jnp.dot(pick, y_ref[e], preferred_element_type=jnp.float32)
    out_ref[...] = acc.astype(out_ref.dtype)


def combine(hidden, pos, probs, y, column):
    toks, dim = hidden.shape
    n, limit, width = y.shape
    return pl.pallas_call(
        combine_kernel,
        out_shape=jax.ShapeDtypeStruct((toks, width), hidden.dtype),
        grid=(toks // TOK_TILE,),
        in_specs=[pl.BlockSpec((TOK_TILE, width), lambda i: (i, 0)), pl.BlockSpec((TOK_TILE, n), lambda i: (i, 0)), pl.BlockSpec((TOK_TILE, n), lambda i: (i, 0)),
                  pl.BlockSpec((n, limit, width), lambda i: (0, 0, 0), pipeline_mode=pl.Buffered(1))],
        out_specs=pl.BlockSpec((TOK_TILE, width), lambda i: (i, 0)),
        cost_estimate=pl.CostEstimate(flops=2 * toks * limit * width * n, bytes_accessed=2 * n * limit * width + 8 * toks * width, transcendentals=0),
        compiler_params=pltpu.CompilerParams(vmem_limit_bytes=VMEM_LIMIT),
        name="combine",
    )(lax.dynamic_slice_in_dim(hidden, column * width, width, axis=1), pos, probs, y)


def solution(mesh):
    chips = mesh.shape["ep"] // 2
    tp_size = mesh.shape["tp"]

    def per_device(hidden, expert_ids, norm_w, router_w, w_gate, w_up, w_down):
        tok_dev = hidden.shape[0]
        top_k = expert_ids.shape[1]
        n_experts = router_w.shape[1]
        row_limit = row_cap(tok_dev, top_k, n_experts)
        experts = jnp.arange(n_experts, dtype=jnp.int32)
        chosen = jnp.sum((expert_ids[:, :, None] == experts).astype(jnp.int32), axis=1)
        pos = jnp.where(chosen > 0, jnp.cumsum(chosen, axis=0) - 1, -1)
        recv_pos = lax.all_to_all(pos.T, "ep", 0, 0, tiled=True)
        normed = rms_norm(hidden, norm_w)
        probs = jax.nn.softmax(jnp.dot(normed, router_w, preferred_element_type=jnp.float32), axis=-1)
        y = experts_apply(chips, tp_size, row_limit, normed, recv_pos, w_gate[0], w_up[0], w_down[0])
        out_cols = combine(hidden, pos, probs, y, lax.axis_index("tp"))
        return lax.all_gather(out_cols, "tp", axis=1, tiled=True)

    token_spec = P(("dp", "ep"), None)
    return jax.shard_map(per_device, mesh=mesh, in_specs=(token_spec, token_spec, P(None), P(None, None), P("ep", None, "tp"), P("ep", None, "tp"), P("ep", "tp", None)), out_specs=token_spec, check_vma=False)
```

```python
import functools

import jax
import jax.numpy as jnp
from jax import lax
from jax.experimental import pallas as pl
from jax.experimental.pallas import tpu as pltpu
from jax.sharding import PartitionSpec as P

NORM_EPS = 1e-6
VMEM_LIMIT = 60 * 1024 * 1024
SLOT_TILE = 256
RING = 4
MESH = pl.DeviceIdType.MESH
BLOCKS = ((0, 0), (0, 1), (-1, 0), (1, 0), (-1, 1), (1, 1), (2, 0), (2, 1))


def rms_norm(hidden, norm_w):
    wide_h = hidden.astype(jnp.float32)
    mean_sq = jnp.mean(wide_h * wide_h, axis=-1, keepdims=True)
    return (wide_h * lax.rsqrt(mean_sq + NORM_EPS) * norm_w.astype(jnp.float32)).astype(jnp.bfloat16)


def row_cap(tok_dev, top_k, n_experts):
    return 8 * ((2 * top_k * tok_dev + 8 * n_experts - 1) // (8 * n_experts))


def norm_kernel(hidden_ref, w_ref, out_ref):
    out_ref[...] = rms_norm(hidden_ref[...], w_ref[...])


def norm_rows(hidden, norm_w):
    toks, dim = hidden.shape
    tile = pl.BlockSpec((SLOT_TILE, dim), lambda i: (i, 0))
    return pl.pallas_call(
        norm_kernel,
        out_shape=jax.ShapeDtypeStruct((toks, dim), jnp.bfloat16),
        grid=(toks // SLOT_TILE,),
        in_specs=[tile, pl.BlockSpec((1, dim), lambda i: (0, 0))],
        out_specs=tile,
        cost_estimate=pl.CostEstimate(flops=6 * toks * dim, bytes_accessed=4 * toks * dim, transcendentals=toks),
        name="norm_rows",
    )(hidden, norm_w.reshape(1, dim))


def remote(src, dst, send, recv, device):
    return pltpu.make_async_remote_copy(src_ref=src, dst_ref=dst, send_sem=send, recv_sem=recv, device_id=device, device_id_type=MESH)


def enter(peers):
    barrier = pltpu.get_barrier_semaphore()
    for peer in peers:
        pl.semaphore_signal(barrier, inc=1, device_id=peer, device_id_type=MESH)
    pl.semaphore_wait(barrier, len(peers))


def expert_kernel(chips, tp_size, v_ref, pos_ref, gate_hbm, up_hbm, down_hbm, vbuf, home,
                  gate_ref, up_ref, down_ref, v_now, pos_now, stage, recv_f, recv_c, recv_d, fin,
                  w_sem, v_sem, part_sem, hop_send, hop_recv, pair_send, pair_recv, fwd_send, fwd_recv,
                  near_send, near_recv, far_send, far_recv,
                  f_send, f_recv, c_send, c_recv, d_send, d_recv, home_send, home_recv, own_sem):
    y = lax.axis_index("tp")
    me = lax.axis_index("ep")
    chip, core = me // 2, me % 2
    row_part, dim = v_ref.shape[2:]
    tok_dev = 2 * tp_size * row_part
    short = row_part // 2
    n_tiles = home.shape[1] // SLOT_TILE
    steps = len(BLOCKS) * n_tiles
    wide = dim // tp_size
    side = wide // 2
    to_ep = lambda dx, c: {"ep": 2 * lax.rem(chip + dx + chips, chips) + c}
    to_tp = lambda dy: {"tp": lax.rem(y + dy + tp_size, tp_size)}
    partner = to_ep(0, 1 - core)

    weights = [pltpu.make_async_copy(a, b, w_sem.at[j]) for j, (a, b) in enumerate(((gate_hbm, gate_ref), (up_hbm, up_ref), (down_hbm, down_ref)))]
    for w in weights:
        w.start()
    enter([to_tp(1), to_tp(-1), partner] + [to_ep(dx, c) for dx in (-1, 1, 2) for c in (0, 1)])

    at = lambda dx, sc: BLOCKS.index((dx, sc)) - 1
    way = lambda sign: (sign + 1) // 2

    def swap(j):
        c = 1 - core if j == 0 else core
        return remote(v_ref.at[:, c], vbuf.at[0, :, c], part_sem.at[0, j], part_sem.at[1, j], partner)

    def swap_arrival(j):
        c = core if j == 0 else 1 - core
        return remote(v_ref.at[:, c], vbuf.at[0, :, c], part_sem.at[0, j], part_sem.at[1, j], partner)

    def hop(sc, sign, own):
        src = v_ref if own else vbuf.at[0]
        part = slice(None) if sc == 0 else y
        return remote(src.at[part, core], vbuf.at[at(-sign, sc), part, core], hop_send.at[sc, way(sign)], hop_recv.at[sc, way(sign)], to_ep(sign, core))

    def near(sign, d, q):
        part = vbuf.at[at(sign, 1), q, core]
        return remote(part, part, near_send.at[way(sign), d], near_recv.at[way(sign), d], to_tp(1 - 2 * d))

    def far(sign, d, q):
        part = vbuf.at[at(sign, 1), q, core, pl.ds(d * short, short)]
        return remote(part, part, far_send.at[way(sign), d], far_recv.at[way(sign), d], to_tp(1 - 2 * d))

    def forward(sc, sign):
        rows = pl.ds(way(-sign) * short, short)
        return remote(vbuf.at[at(-sign, sc), :, core, rows], vbuf.at[at(2, sc), :, core, rows], fwd_send.at[sc, way(sign)], fwd_recv.at[sc, way(sign)], to_ep(sign, core))

    def pair(k):
        return remote(vbuf.at[k - 1, :, core], vbuf.at[k - 1, :, core], pair_send.at[k], pair_recv.at[k], partner)

    def pair_arrival(k):
        return remote(vbuf.at[k - 1, :, 1 - core], vbuf.at[k - 1, :, 1 - core], pair_send.at[k], pair_recv.at[k], partner)

    around = lambda dy: lax.rem(y + dy + tp_size, tp_size)

    swap(0).start()
    swap(1).start()

    @pl.when(core == 0)
    def _():
        swap_arrival(0).wait_recv()
        for sc in (1, 0):
            for sign in (1, -1):
                hop(sc, sign, sc == 0).start()

    @pl.when(core == 1)
    def _():
        for sign in (1, -1):
            hop(1, sign, True).start()
        swap_arrival(0).wait_recv()
        for sign in (1, -1):
            hop(0, sign, False).start()

    def load(src, row):
        copy = pltpu.make_async_copy(src, v_now, v_sem)
        copy.start()
        pos_now[...] = pos_ref[pl.ds(row, 1), :]
        copy.wait()

    def spread():
        for sign in (1, -1):
            hop(1, sign, True).wait_recv()
            for d in (0, 1):
                near(-sign, d, y).start()

    def block_start(k):
        dx, sc = BLOCKS[k]
        if k == 0:
            for w in weights:
                w.wait()
            load(v_ref, me)
            return
        if k == 1:
            swap_arrival(1).wait_recv()
            load(vbuf.at[0], 2 * chip + 1 - core)
            return
        if k == 2:
            for sign in (-1, 1):
                for d in (0, 1):
                    q = around(2 * d - 1)
                    near(sign, d, q).wait_recv()
                    far(sign, d, q).start()
            for sign in (1, -1):
                hop(0, sign, True).wait_recv()
                forward(0, sign).start()
                pair(BLOCKS.index((-sign, 0))).start()
        if k == 3:
            for sign in (1, -1):
                for d in (0, 1):
                    far(-sign, d, around(2)).wait_recv()
                forward(1, sign).start()
                pair(BLOCKS.index((-sign, 1))).start()
        if k in (5, 6):
            for sign in (1, -1):
                forward(k - 5, sign).wait_recv()
            pair(k + 1).start()
        pair_arrival(k).wait_recv()
        load(vbuf.at[k - 1], 2 * lax.rem(chip + dx + chips, chips) + sc)

    def f_copy(s, d):
        return remote(stage.at[s, 3, d], recv_f.at[d, s], f_send.at[d, s], f_recv.at[d, s], to_tp(1 - 2 * d))

    def c_copy(s, d):
        return remote(stage.at[s, 1 + d, d], recv_c.at[d, s], c_send.at[d, s], c_recv.at[d, s], to_tp(1 - 2 * d))

    def d_copy(s, d):
        return remote(stage.at[s, 1 + d, 1 - d], recv_d.at[d, s], d_send.at[d, s], d_recv.at[d, s], to_tp(1 - 2 * d))

    def rows_of(tile):
        return pl.ds(pl.multiple_of(tile * SLOT_TILE, SLOT_TILE), SLOT_TILE)

    def home_copy(k, s, tile):
        dx, sc = BLOCKS[k]
        device = partner if k == 1 else to_ep(dx, sc)
        return remote(fin.at[s], home.at[me, rows_of(tile)], home_send.at[s], home_recv, device)

    def own_copy(s, tile):
        return pltpu.make_async_copy(fin.at[s], home.at[me, rows_of(tile)], own_sem.at[s])

    def step(i, carry):
        @pl.when(i == n_tiles - 1)
        def _():
            spread()

        for k in range(len(BLOCKS)):
            @pl.when(i == k * n_tiles)
            def _(k=k):
                block_start(k)

        @pl.when(i < steps)
        def _():
            s = lax.rem(i, RING)

            @pl.when(i >= RING)
            def _():
                for d in (0, 1):
                    f_copy(s, d).wait_send()
                    c_copy(s, d).wait_send()
                    d_copy(s, d).wait_send()

            slots = lax.rem(i, n_tiles) * SLOT_TILE + lax.broadcasted_iota(jnp.int32, (SLOT_TILE, tok_dev), 0)
            pick = jnp.where(pos_now[...] == slots, 1.0, 0.0).astype(jnp.bfloat16)
            rows = jnp.dot(pick, v_now[...].reshape(tok_dev, dim), preferred_element_type=jnp.float32).astype(jnp.bfloat16)
            gate_pre = jnp.dot(rows, gate_ref[...], preferred_element_type=jnp.float32)
            up_pre = jnp.dot(rows, up_ref[...], preferred_element_type=jnp.float32)
            act = (jax.nn.silu(gate_pre) * up_pre).astype(jnp.bfloat16)
            for part, dy in ((3, 2), (1, 1), (2, -1), (0, 0)):
                q = lax.rem(y + dy + tp_size, tp_size)
                for d in (0, 1):
                    cols = pl.ds(pl.multiple_of(q * wide + d * side, side), side)
                    stage[s, part, d] = jnp.dot(act, down_ref[:, cols], preferred_element_type=jnp.float32).astype(jnp.bfloat16)
            for d in (0, 1):
                f_copy(s, d).start()
            for d in (0, 1):
                d_copy(s, d).start()

        @pl.when(i >= 2)
        def _():
            j = i - 2
            s = lax.rem(j, RING)
            tile = lax.rem(j, n_tiles)
            for d in (0, 1):
                c_copy(s, d).wait_recv()
                d_copy(s, d).wait_recv()

            @pl.when((j >= RING) & (j < RING + n_tiles))
            def _():
                own_copy(s, tile).wait()

            @pl.when(j >= RING + n_tiles)
            def _():
                home_copy(2, s, tile).wait_send()

            f32 = lambda a: a.astype(jnp.float32)
            for d in (0, 1):
                total = f32(stage[s, 0, d]) + f32(recv_c[d, s]) + f32(recv_d[1 - d, s])
                fin[s, :, d * side:(d + 1) * side] = total.astype(jnp.bfloat16)

            @pl.when(j < n_tiles)
            def _():
                own_copy(s, tile).start()

            for k in range(1, len(BLOCKS)):
                @pl.when(j // n_tiles == k)
                def _(k=k):
                    home_copy(k, s, tile).start()

        @pl.when((i >= 1) & (i <= steps))
        def _():
            s = lax.rem(i - 1, RING)
            for d in (0, 1):
                f_copy(s, d).wait_recv()
                stage[s, 1 + d, d] = (stage[s, 1 + d, d].astype(jnp.float32) + recv_f[d, s].astype(jnp.float32)).astype(jnp.bfloat16)
                c_copy(s, d).start()

        return carry

    assert n_tiles == RING
    lax.fori_loop(0, steps + 2, step, 0)

    for s in range(RING):
        for d in (0, 1):
            f_copy(s, d).wait_send()
            c_copy(s, d).wait_send()
            d_copy(s, d).wait_send()
        home_copy(2, s, s).wait_send()
    for j in (0, 1):
        swap(j).wait_send()
    for sc in (0, 1):
        for sign in (1, -1):
            hop(sc, sign, True).wait_send()
            forward(sc, sign).wait_send()
    for sign in (1, -1):
        for d in (0, 1):
            near(sign, d, y).wait_send()
            far(sign, d, y).wait_send()
    for k in range(2, len(BLOCKS)):
        pair(k).wait_send()
    arrived = home.at[pl.ds(0, home.shape[0] - 1)]
    remote(arrived, arrived, home_send.at[0], home_recv, partner).wait_recv()


def experts_apply(chips, tp_size, row_limit, v, pos_rows, gate, up, down):
    tok_dev, dim = v.shape
    ff = gate.shape[1]
    width = dim // tp_size
    side = width // 2
    n = len(BLOCKS)
    bf16 = jnp.bfloat16
    anywhere = pl.BlockSpec(memory_space=pl.ANY)
    dma = pltpu.SemaphoreType.DMA
    ring = (2, RING, SLOT_TILE, side)
    parts = (tp_size, 2, tok_dev // (2 * tp_size), dim)
    return pl.pallas_call(
        functools.partial(expert_kernel, chips, tp_size),
        out_shape=(jax.ShapeDtypeStruct((n - 1, *parts), bf16), jax.ShapeDtypeStruct((n, row_limit, width), bf16)),
        in_specs=[anywhere, pl.BlockSpec(memory_space=pltpu.VMEM), anywhere, anywhere, anywhere],
        out_specs=(anywhere, anywhere),
        scratch_shapes=[
            pltpu.VMEM((dim, ff), bf16), pltpu.VMEM((dim, ff), bf16), pltpu.VMEM((ff, dim), bf16),
            pltpu.VMEM(parts, bf16), pltpu.VMEM((1, tok_dev), jnp.int32),
            pltpu.VMEM((RING, 4, 2, SLOT_TILE, side), bf16), pltpu.VMEM(ring, bf16), pltpu.VMEM(ring, bf16), pltpu.VMEM(ring, bf16),
            pltpu.VMEM((RING, SLOT_TILE, width), bf16),
            dma((3,)), dma, dma((2, 2)), dma((2, 2)), dma((2, 2)), dma((n,)), dma((n,)), dma((2, 2)), dma((2, 2)),
            dma((2, 2)), dma((2, 2)), dma((2, 2)), dma((2, 2)),
            dma((2, RING)), dma((2, RING)), dma((2, RING)), dma((2, RING)), dma((2, RING)), dma((2, RING)),
            dma((RING,)), dma, dma((RING,)),
        ],
        cost_estimate=pl.CostEstimate(flops=2 * n * row_limit * dim * (tok_dev + 3 * ff), bytes_accessed=2 * (n * tok_dev * dim + 3 * dim * ff), transcendentals=n * row_limit * ff),
        compiler_params=pltpu.CompilerParams(collective_id=0, has_side_effects=True, vmem_limit_bytes=VMEM_LIMIT),
        name="experts",
    )(v.reshape(parts), pos_rows, gate, up, down)[1]


def finish_kernel(tp_size, pos_ref, router_ref, y_ref, hidden_hbm, v_hbm, out, hidden_ref, v_ref, done, v_sem, hidden_sem, own_sem, near_send, near_recv, far_send, far_recv):
    y = lax.axis_index("tp")
    width = done.shape[1]
    tiles = done.shape[0] // SLOT_TILE
    short = SLOT_TILE // 2
    to_tp = lambda dy: {"tp": lax.rem(y + dy + tp_size, tp_size)}
    cols = lambda dy: pl.ds(pl.multiple_of(lax.rem(y + dy + tp_size, tp_size) * width, width), width)
    rows_of = lambda t: pl.ds(pl.multiple_of(t * SLOT_TILE, SLOT_TILE), SLOT_TILE)

    fetch_v = lambda t: pltpu.make_async_copy(v_hbm.at[rows_of(t)], v_ref.at[rows_of(t)], v_sem.at[t])
    fetch_h = pltpu.make_async_copy(hidden_hbm.at[:, cols(0)], hidden_ref, hidden_sem)
    fetch_h.start()
    for t in range(tiles):
        fetch_v(t).start()
    enter([to_tp(1), to_tp(-1)])

    own = lambda t: pltpu.make_async_copy(done.at[rows_of(t)], out.at[rows_of(t), cols(0)], own_sem.at[t])

    def near(t, d, dy):
        return remote(done.at[rows_of(t)], out.at[rows_of(t), cols(dy)], near_send.at[d, t], near_recv.at[d, t], to_tp(1 - 2 * d))

    def far(t, d, dy):
        part = out.at[pl.ds(pl.multiple_of(t * SLOT_TILE + d * short, short), short), cols(dy)]
        return remote(part, part, far_send.at[d, t], far_recv.at[d, t], to_tp(1 - 2 * d))

    fetch_h.wait()

    def step(t, carry):
        @pl.when(t < tiles)
        def _():
            fetch_v(t).wait()
            rows = rows_of(t)
            logits = jnp.dot(v_ref[rows, :], router_ref[...], preferred_element_type=jnp.float32)
            probs = jax.nn.softmax(logits, axis=-1)
            acc = hidden_ref[rows, :].astype(jnp.float32)
            pos = pos_ref[rows, :]
            for e in range(y_ref.shape[0]):
                slots = lax.broadcasted_iota(jnp.int32, (SLOT_TILE, y_ref.shape[1]), 1)
                pick = jnp.where(pos[:, e:e + 1] == slots, 1.0, 0.0).astype(jnp.bfloat16)
                acc += probs[:, e:e + 1] * jnp.dot(pick, y_ref[e], preferred_element_type=jnp.float32)
            done[rows, :] = acc.astype(done.dtype)
            own(t).start()
            for d in (0, 1):
                near(t, d, 0).start()

        @pl.when(t >= 1)
        def _():
            for d in (0, 1):
                near(t - 1, d, 2 * d - 1).wait_recv()
                far(t - 1, d, 2 * d - 1).start()

        return carry

    lax.fori_loop(0, tiles + 1, step, 0)
    for t in range(tiles):
        own(t).wait()
        for d in (0, 1):
            near(t, d, 0).wait_send()
            far(t, d, 2 * d - 1).wait_send()
            far(t, d, 2).wait_recv()


def finish(tp_size, hidden, v, pos, router_w, y):
    toks, dim = hidden.shape
    n, limit, width = y.shape
    tiles = toks // SLOT_TILE
    anywhere = pl.BlockSpec(memory_space=pl.ANY)
    vmem = pl.BlockSpec(memory_space=pltpu.VMEM)
    dma = pltpu.SemaphoreType.DMA
    return pl.pallas_call(
        functools.partial(finish_kernel, tp_size),
        out_shape=jax.ShapeDtypeStruct((toks, dim), hidden.dtype),
        in_specs=[vmem, vmem, vmem, anywhere, anywhere],
        out_specs=anywhere,
        scratch_shapes=[pltpu.VMEM((toks, width), hidden.dtype), pltpu.VMEM((toks, dim), v.dtype), pltpu.VMEM((toks, width), hidden.dtype),
                        dma((tiles,)), dma, dma((tiles,)), dma((2, tiles)), dma((2, tiles)), dma((2, tiles)), dma((2, tiles))],
        cost_estimate=pl.CostEstimate(flops=2 * toks * limit * width * n, bytes_accessed=2 * n * limit * width + 8 * toks * width, transcendentals=0),
        compiler_params=pltpu.CompilerParams(collective_id=1, has_side_effects=True, vmem_limit_bytes=VMEM_LIMIT),
        name="finish",
    )(pos, router_w, y, hidden, v)


def solution(mesh):
    chips = mesh.shape["ep"] // 2
    tp_size = mesh.shape["tp"]

    def per_device(hidden, expert_ids, norm_w, router_w, w_gate, w_up, w_down):
        tok_dev = hidden.shape[0]
        top_k = expert_ids.shape[1]
        n_experts = router_w.shape[1]
        row_limit = row_cap(tok_dev, top_k, n_experts)
        experts = jnp.arange(n_experts, dtype=jnp.int32)
        chosen = jnp.sum((expert_ids[:, :, None] == experts).astype(jnp.int32), axis=1)
        pos = jnp.where(chosen > 0, jnp.cumsum(chosen, axis=0) - 1, -1)
        recv_pos = lax.all_to_all(pos.T, "ep", 0, 0, tiled=True)
        normed = norm_rows(hidden, norm_w)
        y = experts_apply(chips, tp_size, row_limit, normed, recv_pos, w_gate[0], w_up[0], w_down[0])
        return finish(tp_size, hidden, normed, pos, router_w, y)

    token_spec = P(("dp", "ep"), None)
    return jax.shard_map(per_device, mesh=mesh, in_specs=(token_spec, token_spec, P(None), P(None, None), P("ep", None, "tp"), P("ep", None, "tp"), P("ep", "tp", None)), out_specs=token_spec, check_vma=False)
```

```python
import functools

import jax
import jax.numpy as jnp
from jax import lax
from jax.experimental import pallas as pl
from jax.experimental.pallas import tpu as pltpu
from jax.sharding import PartitionSpec as P

NORM_EPS = 1e-6
VMEM_LIMIT = 63 * 1024 * 1024
SLOT_TILE = 256
NORM_TILE = 512
RING = 8
FIN = 4
CHAIN = 2
FINAL = 4
MESH = pl.DeviceIdType.MESH
BLOCKS = ((0, 0), (0, 1), (-1, 0), (1, 0), (-1, 1), (1, 1), (2, 0), (2, 1))


def rms_norm(hidden, norm_w):
    wide_h = hidden.astype(jnp.float32)
    mean_sq = jnp.mean(wide_h * wide_h, axis=-1, keepdims=True)
    return (wide_h * lax.rsqrt(mean_sq + NORM_EPS) * norm_w.astype(jnp.float32)).astype(jnp.bfloat16)


def row_cap(tok_dev, top_k, n_experts):
    return 8 * ((2 * top_k * tok_dev + 8 * n_experts - 1) // (8 * n_experts))


def norm_kernel(hidden_ref, w_ref, out_ref):
    out_ref[...] = rms_norm(hidden_ref[...], w_ref[...])


def norm_rows(hidden, norm_w):
    toks, dim = hidden.shape
    tile = pl.BlockSpec((NORM_TILE, dim), lambda i: (i, 0))
    return pl.pallas_call(
        norm_kernel,
        out_shape=jax.ShapeDtypeStruct((toks, dim), jnp.bfloat16),
        grid=(toks // NORM_TILE,),
        in_specs=[tile, pl.BlockSpec((1, dim), lambda i: (0, 0))],
        out_specs=tile,
        cost_estimate=pl.CostEstimate(flops=6 * toks * dim, bytes_accessed=4 * toks * dim, transcendentals=toks),
        name="norm_rows",
    )(hidden, norm_w.reshape(1, dim))


def remote(src, dst, send, recv, device):
    return pltpu.make_async_remote_copy(src_ref=src, dst_ref=dst, send_sem=send, recv_sem=recv, device_id=device, device_id_type=MESH)


def enter(peers):
    barrier = pltpu.get_barrier_semaphore()
    for peer in peers:
        pl.semaphore_signal(barrier, inc=1, device_id=peer, device_id_type=MESH)
    pl.semaphore_wait(barrier, len(peers))


def expert_kernel(chips, tp_size, v_ref, pos_ref, gate_hbm, up_hbm, down_hbm, vbuf, home,
                  gate_ref, up_ref, down_ref, v_now, pos_now, stage, recv_f, recv_c, recv_d, fin,
                  w_sem, v_sem, part_sem, hop_send, hop_recv, pair_send, pair_recv, fwd_send, fwd_recv,
                  near_send, near_recv, far_send, far_recv,
                  f_send, f_recv, c_send, c_recv, d_send, d_recv, home_send, home_recv, own_sem):
    y = lax.axis_index("tp")
    me = lax.axis_index("ep")
    chip, core = me // 2, me % 2
    row_part, dim = v_ref.shape[2:]
    tok_dev = 2 * tp_size * row_part
    short = row_part // 2
    n_tiles = home.shape[1] // SLOT_TILE
    steps = len(BLOCKS) * n_tiles
    wide = dim // tp_size
    side = wide // 2
    to_ep = lambda dx, c: {"ep": 2 * lax.rem(chip + dx + chips, chips) + c}
    to_tp = lambda dy: {"tp": lax.rem(y + dy + tp_size, tp_size)}
    partner = to_ep(0, 1 - core)

    weights = [pltpu.make_async_copy(a, b, w_sem.at[j]) for j, (a, b) in enumerate(((gate_hbm, gate_ref), (up_hbm, up_ref), (down_hbm, down_ref)))]
    for w in weights:
        w.start()
    enter([to_tp(1), to_tp(-1), partner] + [to_ep(dx, c) for dx in (-1, 1, 2) for c in (0, 1)])

    at = lambda dx, sc: BLOCKS.index((dx, sc)) - 1
    way = lambda sign: (sign + 1) // 2

    def swap(j):
        c = 1 - core if j == 0 else core
        return remote(v_ref.at[:, c], vbuf.at[0, :, c], part_sem.at[0, j], part_sem.at[1, j], partner)

    def swap_arrival(j):
        c = core if j == 0 else 1 - core
        return remote(v_ref.at[:, c], vbuf.at[0, :, c], part_sem.at[0, j], part_sem.at[1, j], partner)

    def hop(sc, sign, own):
        src = v_ref if own else vbuf.at[0]
        part = slice(None) if sc == 0 else y
        return remote(src.at[part, core], vbuf.at[at(-sign, sc), part, core], hop_send.at[sc, way(sign)], hop_recv.at[sc, way(sign)], to_ep(sign, core))

    def near(sign, d, q):
        part = vbuf.at[at(sign, 1), q, core]
        return remote(part, part, near_send.at[way(sign), d], near_recv.at[way(sign), d], to_tp(1 - 2 * d))

    def far(sign, d, q):
        part = vbuf.at[at(sign, 1), q, core, pl.ds(d * short, short)]
        return remote(part, part, far_send.at[way(sign), d], far_recv.at[way(sign), d], to_tp(1 - 2 * d))

    def forward(sc, sign):
        rows = pl.ds(way(-sign) * short, short)
        return remote(vbuf.at[at(-sign, sc), :, core, rows], vbuf.at[at(2, sc), :, core, rows], fwd_send.at[sc, way(sign)], fwd_recv.at[sc, way(sign)], to_ep(sign, core))

    def pair(k):
        return remote(vbuf.at[k - 1, :, core], vbuf.at[k - 1, :, core], pair_send.at[k], pair_recv.at[k], partner)

    def pair_arrival(k):
        return remote(vbuf.at[k - 1, :, 1 - core], vbuf.at[k - 1, :, 1 - core], pair_send.at[k], pair_recv.at[k], partner)

    around = lambda dy: lax.rem(y + dy + tp_size, tp_size)

    swap(0).start()
    swap(1).start()

    @pl.when(core == 0)
    def _():
        swap_arrival(0).wait_recv()
        for sc in (1, 0):
            for sign in (1, -1):
                hop(sc, sign, sc == 0).start()

    @pl.when(core == 1)
    def _():
        for sign in (1, -1):
            hop(1, sign, True).start()
        swap_arrival(0).wait_recv()
        for sign in (1, -1):
            hop(0, sign, False).start()

    def load(k):
        src = v_ref if k == 0 else vbuf.at[k - 1]
        return pltpu.make_async_copy(src, v_now.at[k % 2], v_sem.at[k % 2])

    def fetch(k):
        dx, sc = BLOCKS[k]
        if k == 1:
            swap_arrival(1).wait_recv()
        if k > 1:
            pair_arrival(k).wait_recv()
        load(k).start()
        row = (me, 2 * chip + 1 - core)[k] if k < 2 else 2 * lax.rem(chip + dx + chips, chips) + sc
        pos_now[k % 2] = pos_ref[pl.ds(row, 1), :]

    def spread():
        for sign in (1, -1):
            hop(1, sign, True).wait_recv()
            for d in (0, 1):
                near(-sign, d, y).start()

    def block_start(k):
        if k == 0:
            fetch(0)
            for w in weights:
                w.wait()
        if k == 2:
            for sign in (-1, 1):
                for d in (0, 1):
                    q = around(2 * d - 1)
                    near(sign, d, q).wait_recv()
                    far(sign, d, q).start()
            for sign in (1, -1):
                hop(0, sign, True).wait_recv()
                forward(0, sign).start()
                pair(BLOCKS.index((-sign, 0))).start()
            fetch(2)
        if k == 3:
            for sign in (1, -1):
                for d in (0, 1):
                    far(-sign, d, around(2)).wait_recv()
                forward(1, sign).start()
                pair(BLOCKS.index((-sign, 1))).start()
        if k in (5, 6):
            for sign in (1, -1):
                forward(k - 5, sign).wait_recv()
            pair(k + 1).start()
        load(k).wait()

    def f_copy(s, d):
        return remote(stage.at[s, 3, d], recv_f.at[d, s], f_send.at[d, s], f_recv.at[d, s], to_tp(1 - 2 * d))

    def c_copy(s, d):
        return remote(stage.at[s, 1 + d, d], recv_c.at[d, s], c_send.at[d, s], c_recv.at[d, s], to_tp(1 - 2 * d))

    def d_copy(s, d):
        return remote(stage.at[s, 1 + d, 1 - d], recv_d.at[d, s], d_send.at[d, s], d_recv.at[d, s], to_tp(1 - 2 * d))

    def rows_of(tile):
        return pl.ds(pl.multiple_of(tile * SLOT_TILE, SLOT_TILE), SLOT_TILE)

    def home_copy(k, s, tile):
        dx, sc = BLOCKS[k]
        device = partner if k == 1 else to_ep(dx, sc)
        return remote(fin.at[s], home.at[me, rows_of(tile)], home_send.at[s], home_recv, device)

    def own_copy(s, tile):
        return pltpu.make_async_copy(fin.at[s], home.at[me, rows_of(tile)], own_sem.at[s])

    def step(i, carry):
        for k in range(1, len(BLOCKS)):
            if k != 2:
                @pl.when(i == k * n_tiles - 1)
                def _(k=k):
                    fetch(k)

        @pl.when(i == n_tiles - 1)
        def _():
            spread()

        for k in range(len(BLOCKS)):
            @pl.when(i == k * n_tiles)
            def _(k=k):
                block_start(k)

        @pl.when(i < steps)
        def _():
            s = lax.rem(i, RING)

            @pl.when(i >= RING)
            def _():
                for d in (0, 1):
                    f_copy(s, d).wait_send()
                    c_copy(s, d).wait_send()
                    d_copy(s, d).wait_send()

            now = lax.rem(i // n_tiles, 2)
            slots = lax.rem(i, n_tiles) * SLOT_TILE + lax.broadcasted_iota(jnp.int32, (SLOT_TILE, tok_dev), 0)
            pick = jnp.where(pos_now[now] == slots, 1.0, 0.0).astype(jnp.bfloat16)
            rows = jnp.dot(pick, v_now[now].reshape(tok_dev, dim), preferred_element_type=jnp.float32).astype(jnp.bfloat16)
            gate_pre = jnp.dot(rows, gate_ref[...], preferred_element_type=jnp.float32)
            up_pre = jnp.dot(rows, up_ref[...], preferred_element_type=jnp.float32)
            act = (jax.nn.silu(gate_pre) * up_pre).astype(jnp.bfloat16)
            for part, dy in ((3, 2), (1, 1), (2, -1), (0, 0)):
                q = lax.rem(y + dy + tp_size, tp_size)
                cols = pl.ds(pl.multiple_of(q * wide, wide), wide)
                total = jnp.dot(act, down_ref[:, cols], preferred_element_type=jnp.float32).astype(jnp.bfloat16)
                for d in (0, 1):
                    stage[s, part, d] = total[:, d * side:(d + 1) * side]
            for d in (0, 1):
                f_copy(s, d).start()
            for d in (0, 1):
                d_copy(s, d).start()

        @pl.when(i >= FINAL)
        def _():
            j = i - FINAL
            s = lax.rem(j, RING)
            slot = lax.rem(j, FIN)
            tile = lax.rem(j, n_tiles)
            for d in (0, 1):
                c_copy(s, d).wait_recv()
                d_copy(s, d).wait_recv()

            @pl.when((j >= FIN) & (j < FIN + n_tiles))
            def _():
                own_copy(slot, tile).wait()

            @pl.when(j >= FIN + n_tiles)
            def _():
                home_copy(2, slot, tile).wait_send()

            f32 = lambda a: a.astype(jnp.float32)
            for d in (0, 1):
                total = f32(stage[s, 0, d]) + f32(recv_c[d, s]) + f32(recv_d[1 - d, s])
                fin[slot, :, d * side:(d + 1) * side] = total.astype(jnp.bfloat16)

            @pl.when(j < n_tiles)
            def _():
                own_copy(slot, tile).start()

            for k in range(1, len(BLOCKS)):
                @pl.when(j // n_tiles == k)
                def _(k=k):
                    home_copy(k, slot, tile).start()

        @pl.when((i >= CHAIN) & (i < steps + CHAIN))
        def _():
            s = lax.rem(i - CHAIN, RING)
            for d in (0, 1):
                f_copy(s, d).wait_recv()
                stage[s, 1 + d, d] = (stage[s, 1 + d, d].astype(jnp.float32) + recv_f[d, s].astype(jnp.float32)).astype(jnp.bfloat16)
                c_copy(s, d).start()

        return carry

    assert n_tiles == FIN
    lax.fori_loop(0, steps + FINAL, step, 0)

    for s in range(RING):
        for d in (0, 1):
            f_copy(s, d).wait_send()
            c_copy(s, d).wait_send()
            d_copy(s, d).wait_send()
    for s in range(FIN):
        home_copy(2, s, s).wait_send()
    for j in (0, 1):
        swap(j).wait_send()
    for sc in (0, 1):
        for sign in (1, -1):
            hop(sc, sign, True).wait_send()
            forward(sc, sign).wait_send()
    for sign in (1, -1):
        for d in (0, 1):
            near(sign, d, y).wait_send()
            far(sign, d, y).wait_send()
    for k in range(2, len(BLOCKS)):
        pair(k).wait_send()
    arrived = home.at[pl.ds(0, home.shape[0] - 1)]
    remote(arrived, arrived, home_send.at[0], home_recv, partner).wait_recv()


def experts_apply(chips, tp_size, row_limit, v, pos_rows, gate, up, down):
    tok_dev, dim = v.shape
    ff = gate.shape[1]
    width = dim // tp_size
    side = width // 2
    n = len(BLOCKS)
    bf16 = jnp.bfloat16
    anywhere = pl.BlockSpec(memory_space=pl.ANY)
    dma = pltpu.SemaphoreType.DMA
    ring = (2, RING, SLOT_TILE, side)
    parts = (tp_size, 2, tok_dev // (2 * tp_size), dim)
    return pl.pallas_call(
        functools.partial(expert_kernel, chips, tp_size),
        out_shape=(jax.ShapeDtypeStruct((n - 1, *parts), bf16), jax.ShapeDtypeStruct((n, row_limit, width), bf16)),
        in_specs=[anywhere, pl.BlockSpec(memory_space=pltpu.VMEM), anywhere, anywhere, anywhere],
        out_specs=(anywhere, anywhere),
        scratch_shapes=[
            pltpu.VMEM((dim, ff), bf16), pltpu.VMEM((dim, ff), bf16), pltpu.VMEM((ff, dim), bf16),
            pltpu.VMEM((2, *parts), bf16), pltpu.VMEM((2, 1, tok_dev), jnp.int32),
            pltpu.VMEM((RING, 4, 2, SLOT_TILE, side), bf16), pltpu.VMEM(ring, bf16), pltpu.VMEM(ring, bf16), pltpu.VMEM(ring, bf16),
            pltpu.VMEM((FIN, SLOT_TILE, width), bf16),
            dma((3,)), dma((2,)), dma((2, 2)), dma((2, 2)), dma((2, 2)), dma((n,)), dma((n,)), dma((2, 2)), dma((2, 2)),
            dma((2, 2)), dma((2, 2)), dma((2, 2)), dma((2, 2)),
            dma((2, RING)), dma((2, RING)), dma((2, RING)), dma((2, RING)), dma((2, RING)), dma((2, RING)),
            dma((FIN,)), dma, dma((FIN,)),
        ],
        cost_estimate=pl.CostEstimate(flops=2 * n * row_limit * dim * (tok_dev + 3 * ff), bytes_accessed=2 * (n * tok_dev * dim + 3 * dim * ff), transcendentals=n * row_limit * ff),
        compiler_params=pltpu.CompilerParams(collective_id=0, has_side_effects=True, vmem_limit_bytes=VMEM_LIMIT),
        name="experts",
    )(v.reshape(parts), pos_rows, gate, up, down)[1]


def finish_kernel(tp_size, pos_ref, router_ref, y_ref, hidden_hbm, v_hbm, out, hidden_ref, v_ref, done, v_sem, hidden_sem, own_sem, near_send, near_recv, far_send, far_recv):
    y = lax.axis_index("tp")
    width = done.shape[1]
    tiles = done.shape[0] // SLOT_TILE
    short = SLOT_TILE // 2
    to_tp = lambda dy: {"tp": lax.rem(y + dy + tp_size, tp_size)}
    cols = lambda dy: pl.ds(pl.multiple_of(lax.rem(y + dy + tp_size, tp_size) * width, width), width)
    rows_of = lambda t: pl.ds(pl.multiple_of(t * SLOT_TILE, SLOT_TILE), SLOT_TILE)

    fetch_v = lambda t: pltpu.make_async_copy(v_hbm.at[rows_of(t)], v_ref.at[rows_of(t)], v_sem.at[t])
    fetch_h = pltpu.make_async_copy(hidden_hbm.at[:, cols(0)], hidden_ref, hidden_sem)
    fetch_h.start()
    for t in range(tiles):
        fetch_v(t).start()
    enter([to_tp(1), to_tp(-1)])

    own = lambda t: pltpu.make_async_copy(done.at[rows_of(t)], out.at[rows_of(t), cols(0)], own_sem.at[t])

    def near(t, d, dy):
        return remote(done.at[rows_of(t)], out.at[rows_of(t), cols(dy)], near_send.at[d, t], near_recv.at[d, t], to_tp(1 - 2 * d))

    def far(t, d, dy):
        part = out.at[pl.ds(pl.multiple_of(t * SLOT_TILE + d * short, short), short), cols(dy)]
        return remote(part, part, far_send.at[d, t], far_recv.at[d, t], to_tp(1 - 2 * d))

    fetch_h.wait()

    def step(t, carry):
        @pl.when(t < tiles)
        def _():
            fetch_v(t).wait()
            rows = rows_of(t)
            logits = jnp.dot(v_ref[rows, :], router_ref[...], preferred_element_type=jnp.float32)
            probs = jax.nn.softmax(logits, axis=-1)
            acc = hidden_ref[rows, :].astype(jnp.float32)
            pos = pos_ref[rows, :]
            for e in range(y_ref.shape[0]):
                slots = lax.broadcasted_iota(jnp.int32, (SLOT_TILE, y_ref.shape[1]), 1)
                pick = jnp.where(pos[:, e:e + 1] == slots, 1.0, 0.0).astype(jnp.bfloat16)
                acc += probs[:, e:e + 1] * jnp.dot(pick, y_ref[e], preferred_element_type=jnp.float32)
            done[rows, :] = acc.astype(done.dtype)
            own(t).start()
            for d in (0, 1):
                near(t, d, 0).start()

        @pl.when(t >= 1)
        def _():
            for d in (0, 1):
                near(t - 1, d, 2 * d - 1).wait_recv()
                far(t - 1, d, 2 * d - 1).start()

        return carry

    lax.fori_loop(0, tiles + 1, step, 0)
    for t in range(tiles):
        own(t).wait()
        for d in (0, 1):
            near(t, d, 0).wait_send()
            far(t, d, 2 * d - 1).wait_send()
            far(t, d, 2).wait_recv()


def finish(tp_size, hidden, v, pos, router_w, y):
    toks, dim = hidden.shape
    n, limit, width = y.shape
    tiles = toks // SLOT_TILE
    anywhere = pl.BlockSpec(memory_space=pl.ANY)
    vmem = pl.BlockSpec(memory_space=pltpu.VMEM)
    dma = pltpu.SemaphoreType.DMA
    return pl.pallas_call(
        functools.partial(finish_kernel, tp_size),
        out_shape=jax.ShapeDtypeStruct((toks, dim), hidden.dtype),
        in_specs=[vmem, vmem, vmem, anywhere, anywhere],
        out_specs=anywhere,
        scratch_shapes=[pltpu.VMEM((toks, width), hidden.dtype), pltpu.VMEM((toks, dim), v.dtype), pltpu.VMEM((toks, width), hidden.dtype),
                        dma((tiles,)), dma, dma((tiles,)), dma((2, tiles)), dma((2, tiles)), dma((2, tiles)), dma((2, tiles))],
        cost_estimate=pl.CostEstimate(flops=2 * toks * limit * width * n, bytes_accessed=2 * n * limit * width + 8 * toks * width, transcendentals=0),
        compiler_params=pltpu.CompilerParams(collective_id=1, has_side_effects=True, vmem_limit_bytes=VMEM_LIMIT),
        name="finish",
    )(pos, router_w, y, hidden, v)


def solution(mesh):
    chips = mesh.shape["ep"] // 2
    tp_size = mesh.shape["tp"]

    def per_device(hidden, expert_ids, norm_w, router_w, w_gate, w_up, w_down):
        tok_dev = hidden.shape[0]
        top_k = expert_ids.shape[1]
        n_experts = router_w.shape[1]
        row_limit = row_cap(tok_dev, top_k, n_experts)
        experts = jnp.arange(n_experts, dtype=jnp.int32)
        chosen = jnp.sum((expert_ids[:, :, None] == experts).astype(jnp.int32), axis=1)
        pos = jnp.where(chosen > 0, jnp.cumsum(chosen, axis=0) - 1, -1)
        recv_pos = lax.all_to_all(pos.T, "ep", 0, 0, tiled=True)
        normed = norm_rows(hidden, norm_w)
        y = experts_apply(chips, tp_size, row_limit, normed, recv_pos, w_gate[0], w_up[0], w_down[0])
        return finish(tp_size, hidden, normed, pos, router_w, y)

    token_spec = P(("dp", "ep"), None)
    return jax.shard_map(per_device, mesh=mesh, in_specs=(token_spec, token_spec, P(None), P(None, None), P("ep", None, "tp"), P("ep", None, "tp"), P("ep", "tp", None)), out_specs=token_spec, check_vma=False)
```
